32 devices in a mesh: groups: 2 (over x), traces: 16 (over z, y, core).
Axes of the slice: x: 2, y: 2, z: 4, core: 2. Of those that a mesh axis runs over, the one named last changes fastest.
Arguments:
- raw_traces: float32 [8192, 8192], P(('groups', 'traces')), parts along dimension 0, may hold values from -6 to 6
- filter_index: int32 [8192], P(('groups', 'traces')), parts along dimension 0, may hold values from 0 to 255
- channel_order: int32 [512], P('groups'), parts along dimension 0, may hold values from 0 to 255, each once
- wavelets: float32 [256, 256], P('traces'), may hold values from -0.375 to 0.375
- damping: float32 [256], P('traces'), may hold values from 0.02 to 0.5
Outputs:
- deconvolved: float32 [8192, 8192], P(('groups', 'traces')), parts along dimension 0
The draws below stay inside these ranges and needn't reach their ends.
There are 2 independent parts, one for each index of `groups`. The reference program is written for one: setup_inputs(seed, part) draws one part's arguments, and reference() takes and returns one part's arrays. A program takes and returns all parts, laid end to end along the dimension named above; an argument that names none is the same for every part. Nothing has to cross between parts.
Inputs may be any that keep to these rules, and one draw needn't show every extreme that they name: `channel_order`: each of 0 to 255 appears once.
All inputs are finite; a program needn't handle non-finite values.
Results may differ from the reference program's by a relative error of at most 0.00021.
Values sent between devices are 32-bit elements; how exact they have to be, the bound alone decides.
No kernel may reach another device: no remote copies, remote signals or barrier semaphores. Data moves between devices by JAX's collectives and lax.ppermute only.
A program may use at most 192 MiB of HBM per device.

```python
import math
import jax
import jax.numpy as jnp
from jax import lax

L = 8192
FILTERS = 256
FLEN = 256
TR_DEV = 256
TRACES = 4096
N_TRACES = 16


def plant(drawn, own_key, smallest, largest):
    longest = drawn.shape.index(max(drawn.shape))
    spots = []
    for shift in (0, 1):
        where = [jax.random.randint(jax.random.fold_in(own_key, axis), (), 0, length) for axis, length in enumerate(drawn.shape)]
        where[longest] = (where[longest] + shift) % drawn.shape[longest]
        spots.append(tuple(where))
    return drawn.at[spots[0]].set(smallest).at[spots[1]].set(largest)


def block_scale(key, shape, pieces, least, largest):
    factor_of, own = 1.0, jax.random.fold_in(key, 6)
    for dim, blocks in pieces:
        steps = jnp.exp(jax.random.uniform(jax.random.fold_in(own, dim), (blocks,), jnp.float32, least / len(pieces), largest / len(pieces)))
        factor_of = factor_of * jnp.repeat(steps, shape[dim] // blocks).reshape([-1 if axis == dim else 1 for axis in range(len(shape))])
    return factor_of


def centred(key, dims, deviation, bound, pieces=(), kind=jnp.bfloat16):
    loudness = block_scale(key, dims, pieces, -0.22, 0.18) if pieces else 1.0
    array = jax.random.normal(key, dims, jnp.float32) * deviation * loudness
    return jnp.minimum(jnp.maximum(array, -bound), bound).astype(kind)


def setup_inputs(seed: int = 0, part: int = 0) -> dict:
    streams_of = jax.random.split(jax.random.key(seed), 6)
    part_keys = jax.random.split(jax.random.fold_in(streams_of[5], part), 6)
    return {
        "raw_traces": centred(part_keys[0], (TRACES, L), 1.0, 6.0, ((0, 16),), jnp.float32),
        "filter_index": plant(jax.random.randint(part_keys[1], (TRACES,), 0, FILTERS), jax.random.fold_in(part_keys[1], 1), 0, FILTERS - 1).astype(jnp.int32),
        "channel_order": jax.random.permutation(part_keys[2], TR_DEV).astype(jnp.int32),
        "wavelets": centred(streams_of[3], (FILTERS, FLEN), FLEN ** -0.5, 0.375, ((0, 16),), jnp.float32),
        "damping": jnp.clip(jnp.exp(math.log(0.5) - 3.218876 * jax.random.uniform(streams_of[4], (FILTERS,), jnp.float32) ** block_scale(streams_of[4], (FILTERS,), ((0, 16),), -0.2, 0.2)), 0.02, 0.5),
    }


def filter_gains(wavelets, damping):
    padded = jnp.pad(wavelets, ((0, 0), (0, L - FLEN)))
    spectrum = jnp.fft.fft(padded, axis=1)
    spec_re = jnp.real(spectrum)
    spec_im = jnp.imag(spectrum)
    power = spec_re * spec_re + spec_im * spec_im
    level = jnp.mean(power, axis=1, keepdims=True)
    denom = power + damping[:, None] * (level + 1e-6)
    return spec_re / denom, -spec_im / denom


def reference(raw_traces, filter_index, channel_order, wavelets, damping):
    gain_re, gain_im = filter_gains(wavelets, damping)
    blocks = raw_traces.reshape(N_TRACES, TR_DEV, L)
    picks = filter_index.reshape(N_TRACES, TR_DEV)

    def one_block(pair):
        rows, index = pair
        spectrum = jnp.fft.fft(rows, axis=1)
        spec_re = jnp.real(spectrum)
        spec_im = jnp.imag(spectrum)
        pick_re = jnp.take(gain_re, index, axis=0)
        pick_im = jnp.take(gain_im, index, axis=0)
        out_re = spec_re * pick_re - spec_im * pick_im
        out_im = spec_re * pick_im + spec_im * pick_re
        return jnp.real(jnp.fft.ifft(lax.complex(out_re, out_im), axis=1))

    results = lax.map(one_block, (blocks, picks)).reshape(TRACES, L)
    out_rows = jnp.arange(TRACES, dtype=jnp.int32)
    position = (out_rows // TR_DEV) * TR_DEV + jnp.take(channel_order, out_rows % TR_DEV).astype(jnp.int32)
    source = ((position % N_TRACES) * TR_DEV + position // N_TRACES).astype(jnp.int32)
    return jnp.take(results, source, axis=0)
```

```python
import math

import jax
import jax.numpy as jnp
import numpy as np
from jax import lax
from jax.experimental import pallas as pl
from jax.experimental.pallas import tpu as pltpu
from jax.sharding import PartitionSpec as P


LANES = 128
HALF = math.sqrt(0.5)


def angle_tables(length, taps):
    half = length // LANES // 2 + 1
    turn = np.outer(np.arange(half), np.arange(taps)) * (2.0 * np.pi / length)
    twist = np.stack([np.cos(turn), np.sin(turn)]).astype(np.float32)
    spin = np.outer(np.arange(LANES), np.arange(LANES)) * (2.0 * np.pi / LANES)
    cos, sin = np.cos(spin), np.sin(spin)
    block = np.block([[cos, -sin], [sin, cos]]).astype(np.float32)
    high = block.astype(jnp.bfloat16)
    low = (block - high.astype(np.float32)).astype(jnp.bfloat16)
    return twist, high, low


def dft4(re, im, sign):
    ar, ai, br, bi = re[0] + re[2], im[0] + im[2], re[0] - re[2], im[0] - im[2]
    cr, ci, dr, di = re[1] + re[3], im[1] + im[3], re[1] - re[3], im[1] - im[3]
    if sign < 0:
        dr, di = di, -dr
    else:
        dr, di = -di, dr
    return [ar + cr, br + dr, ar - cr, br - dr], [ai + ci, bi + di, ai - ci, bi - di]


def dft8(re, im, sign):
    er, ei = dft4(re[0::2], im[0::2], sign)
    fr, fi = dft4(re[1::2], im[1::2], sign)
    gr, gi = [fr[0]], [fi[0]]
    if sign < 0:
        gr += [(fr[1] + fi[1]) * HALF, fi[2], (fi[3] - fr[3]) * HALF]
        gi += [(fi[1] - fr[1]) * HALF, -fr[2], (fi[3] + fr[3]) * -HALF]
    else:
        gr += [(fr[1] - fi[1]) * HALF, -fi[2], (fr[3] + fi[3]) * -HALF]
        gi += [(fi[1] + fr[1]) * HALF, fr[2], (fr[3] - fi[3]) * HALF]
    return (
        [a + b for a, b in zip(er, gr)] + [a - b for a, b in zip(er, gr)],
        [a + b for a, b in zip(ei, gi)] + [a - b for a, b in zip(ei, gi)],
    )


def real_dft8(x):
    a, e = x[0] + x[4], x[0] - x[4]
    b, f = x[2] + x[6], x[2] - x[6]
    c, p = x[1] + x[5], x[1] - x[5]
    d, q = x[3] + x[7], x[3] - x[7]
    ab, cd = a + b, c + d
    m, n = (p - q) * HALF, (p + q) * HALF
    re = [ab + cd, e + m, a - b, e - m, ab - cd]
    im = [None, -(f + n), d - c, f - n, None]
    return re, im


def real_from8(re, im):
    s, d = re[0] + re[4], re[0] - re[4]
    u, v = s + re[2], s - re[2]
    g, h = re[1] + re[3], im[3] - im[1]
    k, t = re[1] - re[3], im[1] + im[3]
    a, b = d - im[2], d + im[2]
    m, n = (k - t) * HALF, (k + t) * HALF
    return [u + g, a + m, v + h, b - n, u - g, a - m, v - h, b + n]


def turn_by(re, im, step, period, sign, scale=1.0):
    angle = sign * 2.0 * math.pi * step / period
    c, s = scale * math.cos(angle), scale * math.sin(angle)
    if step == 0:
        return (re, im) if scale == 1.0 else (re * c, im * c)
    if im is None:
        return re * c, re * s
    return re * c - im * s, re * s + im * c


def three_pass(rows_ref, high_ref, low_ref, to_ref):
    rows = rows_ref[...]
    high = rows.astype(jnp.bfloat16)
    low = (rows - high.astype(jnp.float32)).astype(jnp.bfloat16)
    dot = lambda a, b: jnp.dot(a, b, preferred_element_type=jnp.float32)
    to_ref[...] = dot(high, high_ref[...]) + (dot(low, high_ref[...]) + dot(high, low_ref[...]))


def gain_kernel(pick_ref, bank_ref, twist_ref, high_ref, low_ref, gain_ref, own_ref, lhs_ref, spec_ref):
    step = pl.program_id(0)
    rows = own_ref.shape[0]
    taps = twist_ref.shape[2]
    bins = twist_ref.shape[1]
    scale = 1.0 / ((bins - 1) * 2 * LANES)
    for r in range(rows):
        own_ref[pl.ds(r, 1), :] = bank_ref[pl.ds(pick_ref[step * rows + r], 1), :]
    parts = [own_ref[:, b * LANES : (b + 1) * LANES] for b in range(taps // LANES)]
    level = sum(jnp.sum(w * w, axis=1, keepdims=True) for w in parts)
    floor = own_ref[:, taps : taps + LANES] * (level + 1e-06)
    for k in range(bins):
        at = slice(k * rows, (k + 1) * rows)
        for trig, lane in ((0, 0), (1, LANES)):
            terms = [w * twist_ref[trig, k : k + 1, b * LANES : (b + 1) * LANES] for b, w in enumerate(parts)]
            total = sum(terms[1:], terms[0])
            lhs_ref[at, lane : lane + LANES] = -total if trig else total
    three_pass(lhs_ref, high_ref, low_ref, spec_ref)
    for k in range(bins):
        at = slice(k * rows, (k + 1) * rows)
        re, im = spec_ref[at, :LANES], spec_ref[at, LANES:]
        part = scale / (re * re + im * im + floor)
        gain_ref[0, at, :LANES] = re * part
        gain_ref[0, at, LANES:] = im * part


def trace_kernel(source_ref, place_ref, *refs):
    x_ref, gain_ref, twist_ref, high_ref, low_ref = refs[:5]
    out_ref, mid_ref, lhs_ref, spec_ref, done_ref, sems = refs[-6:]
    rows = x_ref.shape[0]
    bins = twist_ref.shape[1]
    many = place_ref.shape[0] // rows

    def put(k, re, im):
        at = slice(k * rows, (k + 1) * rows)
        c, s = twist_ref[0, k : k + 1, :LANES], twist_ref[1, k : k + 1, :LANES]
        if im is None:
            lhs_ref[at, :LANES] = re * c
            lhs_ref[at, LANES:] = -(re * s)
        else:
            lhs_ref[at, :LANES] = re * c + im * s
            lhs_ref[at, LANES:] = im * c - re * s

    for b in range(8):
        tiles = [x_ref[:, (8 * a + b) * LANES : (8 * a + b + 1) * LANES] for a in range(8)]
        re, im = real_dft8(tiles)
        for c in range(5):
            tr, ti = turn_by(re[c], im[c], b * c, 64, -1.0)
            mid_ref[2 * (8 * c + b)] = tr
            if c:
                mid_ref[2 * (8 * c + b) + 1] = ti if ti is not None else jnp.zeros_like(tr)
    zero = [mid_ref[2 * b] for b in range(8)]
    re, im = real_dft8(zero)
    for d in range(5):
        put(8 * d, re[d], im[d])
    for c in range(1, 5):
        re = [mid_ref[2 * (8 * c + b)] for b in range(8)]
        im = [mid_ref[2 * (8 * c + b) + 1] for b in range(8)]
        re, im = dft8(re, im, -1.0)
        for d in range(8):
            k = c + 8 * d
            if k < bins:
                put(k, re[d], im[d])
            elif c < 4:
                put(64 - k, re[d], -im[d])
    three_pass(lhs_ref, high_ref, low_ref, spec_ref)
    for k in range(bins):
        at = slice(k * rows, (k + 1) * rows)
        xr, xi = spec_ref[at, :LANES], spec_ref[at, LANES:]
        gr, gi = gain_ref[0, at, :LANES], gain_ref[0, at, LANES:]
        lhs_ref[at, :LANES] = xr * gr + xi * gi
        lhs_ref[at, LANES:] = xr * gi - xi * gr
    three_pass(lhs_ref, high_ref, low_ref, spec_ref)

    def get(k):
        at = slice(k * rows, (k + 1) * rows)
        c, s = twist_ref[0, k : k + 1, :LANES], twist_ref[1, k : k + 1, :LANES]
        br, bi = spec_ref[at, :LANES], spec_ref[at, LANES:]
        return br * c + bi * s, br * s - bi * c

    def get_any(k):
        if k < bins:
            return get(k)
        re, im = get(64 - k)
        return re, -im

    for c in range(5):
        if c == 0:
            five = [get(8 * d) for d in range(5)]
            vr = real_from8(
                [re * (2.0 if 0 < d < 4 else 1.0) for d, (re, _) in enumerate(five)],
                [im * 2.0 for _, im in five],
            )
            vi = [None] * 8
        else:
            pairs = [get_any(c + 8 * d) for d in range(8)]
            vr, vi = dft8([p[0] for p in pairs], [p[1] for p in pairs], 1.0)
        for b in range(8):
            tr, ti = (vr[b], None) if c == 0 else turn_by(vr[b], vi[b], b * c, 64, 1.0, 1.0 if c == 4 else 2.0)
            mid_ref[2 * (8 * c + b)] = tr
            if 0 < c < 4:
                mid_ref[2 * (8 * c + b) + 1] = ti
    for b in range(8):
        re = [mid_ref[2 * (8 * c + b)] for c in range(5)]
        im = [None] + [mid_ref[2 * (8 * c + b) + 1] for c in range(1, 4)] + [None]
        for a, y in enumerate(real_from8(re, im)):
            done_ref[:, (8 * a + b) * LANES : (8 * a + b + 1) * LANES] = y

    def move(r):
        to = place_ref[r * many + source_ref[0]]
        return pltpu.make_async_copy(done_ref.at[pl.ds(r, 1), :], out_ref.at[pl.ds(to, 1), :], sems.at[r])

    for r in range(rows):
        move(r).start()
    for r in range(rows):
        move(r).wait()


def all_gains(picks, bank, twist, high, low, rows):
    bins = twist.shape[1]
    sources = picks.shape[0] // rows
    whole = lambda a: pl.BlockSpec(a.shape, lambda i, p: (0,) * a.ndim)
    wide = (bins * rows, 2 * LANES)
    return pl.pallas_call(
        gain_kernel,
        grid_spec=pltpu.PrefetchScalarGridSpec(
            num_scalar_prefetch=1,
            grid=(sources,),
            in_specs=[whole(bank), whole(twist), whole(high), whole(low)],
            out_specs=pl.BlockSpec((1,) + wide, lambda i, p: (i, 0, 0)),
            scratch_shapes=[
                pltpu.VMEM((rows, bank.shape[1]), jnp.float32),
                pltpu.VMEM(wide, jnp.float32),
                pltpu.VMEM(wide, jnp.float32),
            ],
        ),
        out_shape=jax.ShapeDtypeStruct((sources,) + wide, jnp.float32),
        name="gains",
    )(picks, bank, twist, high, low)


def filtered(source, places, chunk, gains, twist, high, low, out):
    rows, length = chunk.shape
    bins = twist.shape[1]
    wide = (bins * rows, 2 * LANES)
    whole = lambda a: pl.BlockSpec(a.shape, lambda i, s, p: (0,) * a.ndim)
    given = [chunk, gains, twist, high, low]
    specs = [
        whole(chunk),
        pl.BlockSpec((1,) + wide, lambda i, s, p: (s[0], 0, 0)),
        whole(twist),
        whole(high),
        whole(low),
    ]
    aliases = {}
    if out is not None:
        aliases = {2 + len(given): 0}
        given.append(out)
        specs.append(pl.BlockSpec(memory_space=pl.ANY))
    return pl.pallas_call(
        trace_kernel,
        grid_spec=pltpu.PrefetchScalarGridSpec(
            num_scalar_prefetch=2,
            grid=(1,),
            in_specs=specs,
            out_specs=pl.BlockSpec(memory_space=pl.ANY),
            scratch_shapes=[
                pltpu.VMEM((80, rows, LANES), jnp.float32),
                pltpu.VMEM(wide, jnp.float32),
                pltpu.VMEM(wide, jnp.float32),
                pltpu.VMEM((rows, length), jnp.float32),
                pltpu.SemaphoreType.DMA((rows,)),
            ],
        ),
        out_shape=jax.ShapeDtypeStruct((places.shape[0], length), jnp.float32),
        input_output_aliases=aliases,
        name="filtered",
    )(source, places, *given)


def hop_table(devices):
    near = math.gcd(devices, 4)
    at = np.arange(devices)
    hops = sorted(range(1, devices), key=lambda s: (s % near, s // near))
    ways = [((at // near + s // near) * near % devices) + ((at % near) ^ (s % near)) for s in hops]
    return np.stack(ways, axis=1).astype(np.int32)


def local(raw_traces, filter_index, channel_order, wavelets, damping):
    held, length = raw_traces.shape
    taps = wavelets.shape[1]
    devices = lax.axis_size("traces")
    here = lax.axis_index("traces")
    rows = held // devices
    twist, high, low = (jnp.asarray(t) for t in angle_tables(length, taps))

    flat = jnp.concatenate([wavelets.reshape(-1), damping, filter_index.astype(jnp.float32)])
    flat = jnp.pad(flat, (0, -flat.size % (8 * LANES))).reshape(-1, LANES)
    known = lax.all_gather(flat, "traces", axis=0, tiled=True).reshape(devices, -1)
    count = wavelets.size
    bank = known[:, :count].reshape(-1, taps)
    level = known[:, count : count + damping.shape[0]].reshape(-1, 1)
    bank = jnp.concatenate([bank, jnp.broadcast_to(level, (level.shape[0], LANES))], axis=1)
    mine = lax.dynamic_slice(known, (0, count + damping.shape[0] + here * rows), (devices, rows))
    picks = mine.astype(jnp.int32).reshape(-1)

    spots = lax.broadcasted_iota(jnp.int32, (held, held), 1)
    match = channel_order[None, :] == lax.broadcasted_iota(jnp.int32, (held, held), 0)
    places = jnp.sum(jnp.where(match, spots, 0), axis=1)

    def block(to):
        return lax.dynamic_slice(raw_traces, (to * rows, 0), (rows, length))

    sends = hop_table(devices)
    takes = np.argsort(sends, axis=0).astype(np.int32)
    ways = lax.dynamic_index_in_dim(jnp.asarray(sends), here, 0, keepdims=False)
    froms = lax.dynamic_index_in_dim(jnp.asarray(takes), here, 0, keepdims=False)
    arrived = [(here.reshape(1), block(here))]
    for hop in range(devices - 1):
        pairs = list(enumerate(sends[:, hop].tolist()))
        arrived.append((froms[hop : hop + 1], lax.ppermute(block(ways[hop]), "traces", pairs)))

    gains = all_gains(picks, bank, twist, high, low, rows)
    out = None
    for source, chunk in arrived:
        out = filtered(source, places, chunk, gains, twist, high, low, out)
    return out


def solution(mesh):
    placed = (
        P(("groups", "traces"), None),
        P(("groups", "traces")),
        P("groups"),
        P("traces", None),
        P("traces"),
    )
    return jax.shard_map(
        local, mesh=mesh, in_specs=placed, out_specs=P(("groups", "traces"), None), check_vma=False
    )
```
